32 devices in a mesh: ov: 16 (over z, y, core), vec: 2 (over x).
Axes of the slice: x: 2, y: 2, z: 4, core: 2. Of those that a mesh axis runs over, the one named last changes fastest.
Arguments:
- chol_vectors: bfloat16 [196608, 4096], P('ov', 'vec'), may hold values from -3.5 to 3.5
- amplitudes: bfloat16 [196608, 256], P('ov'), may hold values from -0.013671875 to 0.013671875
- sigma_prior: bfloat16 [196608, 256], P(('ov', 'vec')), may hold values from -4 to 4
Outputs:
- sigma_cycle: bfloat16 [196608, 256], P(('ov', 'vec'))
The draws below stay inside these ranges and needn't reach their ends.
All inputs are finite; a program needn't handle non-finite values.
Results may differ from the reference program's by a relative error of at most 0.0065.
Values may be sent and summed in bfloat16 or wider, within the bound.
A program may use at most 128 MiB of HBM per device.

```python
import jax
import jax.numpy as jnp
from jax import lax

OV = 196608
NV = 4096
JB = 256


def with_spikes(values, key, source, target, parts, factor):
    def block_of(dim):
        return (jnp.arange(values.shape[dim]) // (values.shape[dim] // parts)).reshape((-1,) + (1,) * (values.ndim - 1 - dim))

    one_side = jax.random.permutation(key, parts)[block_of(target)]
    second = (block_of(target) + parts // 2) % parts
    return jnp.where((block_of(source) == one_side) | (block_of(source) == second), factor * values, values)


def steps_of(key, dims, cuts, low, high):
    gain, own = 1.0, jax.random.fold_in(key, 6)
    for axis_at, blocks in cuts:
        draws = jnp.exp(jax.random.uniform(jax.random.fold_in(own, axis_at), (blocks,), jnp.float32, low / len(cuts), high / len(cuts)))
        gain = gain * jnp.repeat(draws, dims[axis_at] // blocks).reshape([-1 if axis == axis_at else 1 for axis in range(len(dims))])
    return gain


def bell_draw(own_key, shape, deviation, bound, pieces=(), held_as=jnp.bfloat16):
    gain = steps_of(own_key, shape, pieces, -0.22, 0.18) if pieces else 1.0
    result = jax.random.normal(own_key, shape, jnp.float32) * deviation * gain
    return jnp.minimum(jnp.maximum(result, -bound), bound).astype(held_as)


def gaussian_with(rng, extent, width, reach, cuts, heavy, dtype=jnp.bfloat16):
    values = width * jax.random.normal(rng, extent, jnp.float32)
    if cuts:
        values = values * steps_of(rng, extent, cuts, -0.22, 0.18)
    return jnp.clip(with_spikes(values, jax.random.fold_in(rng, 3), *heavy), -reach, reach).astype(dtype)


def setup_inputs(seed: int = 0) -> dict:
    splits = jax.random.split(jax.random.key(seed), 4)
    chol_vectors = gaussian_with(splits[0], (OV, NV), 0.177, 3.5, ((0, 16), (1, 2)), (1, 0, 16, 2.0))
    amplitudes = bell_draw(splits[1], (OV, JB), OV ** -0.5, 0.013671875, ((0, 16),))
    sigma_prior = bell_draw(splits[2], (OV, JB), 0.5, 4.0, ((0, 32),))
    return {"chol_vectors": chol_vectors, "amplitudes": amplitudes, "sigma_prior": sigma_prior}


def reference(chol_vectors, amplitudes, sigma_prior):
    contract = (((0,), (0,)), ((), ()))
    coupling = lax.dot_general(chol_vectors, amplitudes, contract, preferred_element_type=jnp.float32)
    coupling_bf = coupling.astype(jnp.bfloat16)
    cycle = jnp.dot(chol_vectors, coupling_bf, preferred_element_type=jnp.float32)
    return (sigma_prior.astype(jnp.float32) + cycle).astype(jnp.bfloat16)
```

```python
import functools

import jax
import jax.numpy as jnp
from jax import lax
from jax.experimental import pallas as pl
from jax.experimental.pallas import tpu as pltpu
from jax.sharding import PartitionSpec as P

MESH = pl.DeviceIdType.MESH
JT_ROWS = 16
CHUNK = 512
RING = 6
TILE_RING = 6


def halved(size, most):
    while size > most and size % 2 == 0:
        size //= 2
    return size


def divisor(size, choices):
    for choice in choices:
        if size % choice == 0:
            return choice
    return size


def kernel(
    plan, chol, amplitudes, prior, out,
    abuf, at, lbuf, acc, part, paired, halves, arrived, own, coup, weights, tiles, sbuf, rbuf, pbuf,
    a_sems, l_sems, t_sems, p_sem, swap_s, swap_r, scat_s, scat_r, gath_s, gath_r, on_s, on_r, x_s, x_r,
):
    n, groups, H, NC, NB, RB, VC, PV, JW, TR, NT = plan
    half = n // 2
    me = lax.axis_index("ov")
    vec = lax.axis_index("vec")
    side = lax.rem(me, 2)
    group = me // 2
    twin = me + 1 - 2 * side
    rows_out = TR * NT
    JT = JW // JT_ROWS
    VT = n // JT

    def mate(step):
        return 2 * lax.rem(group + step, half) + side

    def origin(step):
        return lax.rem(group + half - step, half)

    def l_copy(i):
        c, b = i // NB, lax.rem(i, NB)
        return pltpu.make_async_copy(
            chol.at[pl.ds(pl.multiple_of(b * RB, RB), RB), pl.ds(pl.multiple_of(c * VC, VC), VC)],
            lbuf.at[lax.rem(i, RING)],
            l_sems.at[lax.rem(i, RING)],
        )

    def a_copy(b):
        return pltpu.make_async_copy(
            amplitudes.at[pl.ds(pl.multiple_of(b * RB, RB), RB), :], abuf.at[b], a_sems.at[b]
        )

    total = NC * NB
    shares = NT * (groups - 1)
    jobs = H * (shares + NT)

    def job_row(q):
        final = q >= H * shares
        k = lax.rem(q, shares)
        t = jnp.where(final, lax.rem(q - H * shares, NT), k // (groups - 1))
        d = jnp.where(final, 0, lax.rem(k, groups - 1) + 1)
        return lax.rem(vec + d, groups) * rows_out + t * TR

    def t_copy(q):
        slot = lax.rem(q, TILE_RING)
        return pltpu.make_async_copy(
            chol.at[pl.ds(pl.multiple_of(job_row(q), TR), TR), :], tiles.at[slot], t_sems.at[slot]
        )

    barrier = pltpu.get_barrier_semaphore()
    pl.semaphore_signal(barrier, inc=1, device_id={"ov": twin}, device_id_type=MESH)

    @pl.loop(1, half)
    def _(step):
        pl.semaphore_signal(barrier, inc=1, device_id={"ov": mate(step)}, device_id_type=MESH)

    @pl.loop(1, groups)
    def _(d):
        pl.semaphore_signal(
            barrier, inc=1, device_id={"vec": lax.rem(vec + d, groups)}, device_id_type=MESH
        )

    for b in range(NB):
        a_copy(b).start()
        if b < min(RING, total):
            l_copy(jnp.int32(b)).start()
    for i in range(NB, min(RING, total)):
        l_copy(jnp.int32(i)).start()

    def compute(c, first, last):
        @pl.loop(first, last)
        def _(b):
            i = c * NB + b
            if c == 0:
                a_copy(b).wait()
                at[b] = abuf[b].T
            l_copy(i).wait()
            acc[...] += jnp.dot(at[b], lbuf[lax.rem(i, RING)], preferred_element_type=jnp.float32)

            @pl.when(i + RING < total)
            def _():
                l_copy(i + RING).start()

    def store_part(c):
        for h in range(H):
            for vt in range(VT):
                block = acc[h * JW : (h + 1) * JW, vt * PV : (vt + 1) * PV]
                part[h, c, vt * JT : (vt + 1) * JT] = block.reshape(JT, JT_ROWS, PV)

    def swap(h, c):
        return pltpu.make_async_remote_copy(
            src_ref=part.at[h, c, pl.ds((1 - side) * half, half)],
            dst_ref=paired.at[h, c],
            send_sem=swap_s.at[h, c],
            recv_sem=swap_r.at[h, c],
            device_id={"ov": twin},
            device_id_type=MESH,
        )

    def scatter(h, c, step):
        return pltpu.make_async_remote_copy(
            src_ref=halves.at[h, c, lax.rem(group + step, half)],
            dst_ref=arrived.at[h, c, step],
            send_sem=scat_s.at[h, c, step],
            recv_sem=scat_r.at[h, c, step],
            device_id={"ov": mate(step)},
            device_id_type=MESH,
        )

    def gather(h, c, step, at_piece):
        return pltpu.make_async_remote_copy(
            src_ref=coup.at[h, c, side * half + at_piece],
            dst_ref=coup.at[h, c, side * half + at_piece],
            send_sem=gath_s.at[h, c, step],
            recv_sem=gath_r.at[h, c, step],
            device_id={"ov": mate(step)},
            device_id_type=MESH,
        )

    def onward(h, c, step, hand):
        return pltpu.make_async_remote_copy(
            src_ref=coup.at[h, c, hand * half + origin(step)],
            dst_ref=coup.at[h, c, hand * half + origin(step)],
            send_sem=on_s.at[h, c, step],
            recv_sem=on_r.at[h, c, step],
            device_id={"ov": twin},
            device_id_type=MESH,
        )

    def step1(h, c):
        swap(h, c).start()

    def step2(h, c):
        swap(h, c).wait_recv()

        @pl.loop(1, half)
        def _(step):
            piece = lax.rem(group + step, half)
            halves[h, c, piece] = (part[h, c, side * half + piece] + paired[h, c, piece]).astype(halves.dtype)
            scatter(h, c, step).start()

        own[h, c] = part[h, c, side * half + group] + paired[h, c, group]

    def step3(h, c):
        @pl.loop(1, half)
        def _(step):
            scatter(h, c, step).wait_recv()
            own[h, c] += arrived[h, c, step].astype(jnp.float32)

        coup[h, c, side * half + group] = own[h, c].astype(coup.dtype)

        @pl.loop(1, half)
        def _(step):
            gather(h, c, step, group).start()

        onward(h, c, 0, side).start()

    def step4(h, c):
        @pl.loop(1, half)
        def _(step):
            gather(h, c, step, origin(step)).wait_recv()
            onward(h, c, step, side).start()

    def step5(h, c):
        @pl.loop(0, half)
        def _(step):
            onward(h, c, step, 1 - side).wait_recv()

        for vt in range(VT):
            block = coup[h, c, vt * JT : (vt + 1) * JT].reshape(JW, PV)
            weights[h, c * VC + vt * PV : c * VC + (vt + 1) * PV, :] = block.T

    early, late = NB // 2, (3 * NB) // 4
    for c in range(NC):
        acc[...] = jnp.zeros_like(acc)
        compute(c, 0, early)
        if c >= 1:
            step2(0, c - 1)
        compute(c, early, late)
        if c >= 2:
            step3(0, c - 2)
        compute(c, late, NB)
        if c >= 3:
            step4(0, c - 3)
        store_part(c)
        if c == 0:
            pl.semaphore_wait(barrier, half + groups - 1)
        step1(0, c)

    for q in range(min(TILE_RING, jobs)):
        t_copy(jnp.int32(q)).start()
    p_copy = pltpu.make_async_copy(prior, pbuf, p_sem)
    p_copy.start()

    late_steps = []
    for c in range(NC):
        if c >= NC - 1:
            late_steps.append((1, step2, c))
        if c >= NC - 2:
            late_steps.append((2 + 2 * (c - NC + 2), step3, c))
        if c >= NC - 3:
            late_steps.append((3 + 2 * (c - NC + 2), step4, c))
    for _, run, c in sorted(late_steps, key=lambda item: item[0]):
        run(0, c)
    for c in range(NC):
        step5(0, c)

    def x_copy(h, d, t, target):
        return pltpu.make_async_remote_copy(
            src_ref=sbuf.at[h, d - 1, t],
            dst_ref=rbuf.at[h, d - 1, t],
            send_sem=x_s.at[h, d - 1, t],
            recv_sem=x_r.at[h, d - 1, t],
            device_id={"vec": target},
            device_id_type=MESH,
        )

    def tile_product(h, q):
        t_copy(q).wait()
        product = jnp.dot(
            tiles[lax.rem(q, TILE_RING)], weights[h], preferred_element_type=jnp.float32
        )
        return product

    def refill(q):
        @pl.when(q + TILE_RING < jobs)
        def _():
            t_copy(q + TILE_RING).start()

    def share_tiles(h, first, last):
        @pl.loop(first, last)
        def _(t):
            for d in range(1, groups):
                q = h * shares + t * (groups - 1) + d - 1
                sbuf[h, d - 1, t] = tile_product(h, q).astype(sbuf.dtype)
                x_copy(h, d, t, lax.rem(vec + d, groups)).start()
                refill(q)

    def final_tiles(h):
        @pl.loop(0, NT)
        def _(t):
            q = H * shares + h * NT + t
            total_tile = tile_product(h, q)
            refill(q)
            rows = pl.ds(pl.multiple_of(t * TR, TR), TR)
            columns = slice(h * JW, (h + 1) * JW)
            for d in range(1, groups):
                x_copy(h, d, t, lax.rem(vec + d, groups)).wait_recv()
                total_tile += rbuf[h, d - 1, t].astype(jnp.float32)
            out[rows, columns] = (pbuf[rows, columns].astype(jnp.float32) + total_tile).astype(out.dtype)

    for h in range(H):
        if h + 1 < H:
            for c in range(NC):
                step1(h + 1, c)
            edges = [0, NT // 8, NT // 2, (3 * NT) // 4, NT]
            for k, run in enumerate((step2, step3, step4, step5)):
                share_tiles(h, edges[k], edges[k + 1])
                for c in range(NC):
                    run(h + 1, c)
        else:
            share_tiles(h, 0, NT)
    p_copy.wait()
    for h in range(H):
        final_tiles(h)

    for h in range(H):
        for c in range(NC):
            swap(h, c).wait_send()

            @pl.loop(1, half)
            def _(step):
                scatter(h, c, step).wait_send()
                gather(h, c, step, group).wait_send()

            @pl.loop(0, half)
            def _(step):
                onward(h, c, step, side).wait_send()

        for d in range(1, groups):

            @pl.loop(0, NT)
            def _(t):
                x_copy(h, d, t, lax.rem(vec + d, groups)).wait_send()


def body(n, groups, chol, amplitudes, prior):
    rows, vectors = chol.shape
    columns = amplitudes.shape[1]
    half = n // 2
    VC = divisor(vectors, (CHUNK, 256, 128))
    H = 2 if VC * (columns // 2) // JT_ROWS // n >= 128 else 1
    NC = vectors // VC
    RB = halved(rows, 2048)
    NB = rows // RB
    JW = columns // H
    PV = VC * (JW // JT_ROWS) // n
    TR = divisor(prior.shape[0], (256, 128, 64, 32, 16))
    NT = prior.shape[0] // TR
    plan = (n, groups, H, NC, NB, RB, VC, PV, JW, TR, NT)
    bf16, f32 = jnp.bfloat16, jnp.float32
    dma = pltpu.SemaphoreType.DMA
    return pl.pallas_call(
        functools.partial(kernel, plan),
        out_shape=jax.ShapeDtypeStruct(prior.shape, prior.dtype),
        in_specs=[pl.BlockSpec(memory_space=pl.ANY)] * 3,
        out_specs=pl.BlockSpec(memory_space=pltpu.VMEM),
        scratch_shapes=[
            pltpu.VMEM((NB, RB, columns), bf16),
            pltpu.VMEM((NB, columns, RB), bf16),
            pltpu.VMEM((RING, RB, VC), bf16),
            pltpu.VMEM((columns, VC), f32),
            pltpu.VMEM((H, NC, n, JT_ROWS, PV), f32),
            pltpu.VMEM((H, NC, half, JT_ROWS, PV), f32),
            pltpu.VMEM((H, NC, half, JT_ROWS, PV), bf16),
            pltpu.VMEM((H, NC, half, JT_ROWS, PV), bf16),
            pltpu.VMEM((H, NC, JT_ROWS, PV), f32),
            pltpu.VMEM((H, NC, n, JT_ROWS, PV), bf16),
            pltpu.VMEM((H, vectors, JW), bf16),
            pltpu.VMEM((TILE_RING, TR, vectors), bf16),
            pltpu.VMEM((H, groups - 1, NT, TR, JW), bf16),
            pltpu.VMEM((H, groups - 1, NT, TR, JW), bf16),
            pltpu.VMEM(prior.shape, bf16),
            dma((NB,)),
            dma((RING,)),
            dma((TILE_RING,)),
            dma(()),
            dma((H, NC)),
            dma((H, NC)),
        ]
        + [dma((H, NC, half))] * 6
        + [dma((H, groups - 1, NT))] * 2,
        compiler_params=pltpu.CompilerParams(
            collective_id=0, has_side_effects=True, vmem_limit_bytes=61 * 2**20
        ),
    )(chol, amplitudes, prior)


def solution(mesh):
    return jax.shard_map(
        functools.partial(body, mesh.shape["ov"], mesh.shape["vec"]),
        mesh=mesh,
        in_specs=(P("ov", "vec"), P("ov", None), P(("ov", "vec"), None)),
        out_specs=P(("ov", "vec"), None),
        check_vma=False,
    )
```

```python
import functools

import jax
import jax.numpy as jnp
from jax import lax
from jax.experimental import pallas as pl
from jax.experimental.pallas import tpu as pltpu
from jax.sharding import PartitionSpec as P

MESH = pl.DeviceIdType.MESH
JT_ROWS = 16
CHUNK = 512
RING = 3
TILE_RING = 6


def halved(size, most):
    while size > most and size % 2 == 0:
        size //= 2
    return size


def divisor(size, choices):
    for choice in choices:
        if size % choice == 0:
            return choice
    return size


def kernel(
    plan, chol, amplitudes, prior, out,
    abuf, at, lbuf, acc, part, paired, halves, arrived, own, coup, weights, tiles, sbuf, rbuf, pbuf,
    a_sems, l_sems, t_sems, p_sem, swap_s, swap_r, scat_s, scat_r, gath_s, gath_r, on_s, on_r, x_s, x_r,
):
    n, groups, H, NC, NB, RB, VC, PV, JW, TR, NT = plan
    half = n // 2
    me = lax.axis_index("ov")
    vec = lax.axis_index("vec")
    side = lax.rem(me, 2)
    group = me // 2
    twin = me + 1 - 2 * side
    rows_out = TR * NT
    JT = JW // JT_ROWS
    VT = n // JT

    def mate(step):
        return 2 * lax.rem(group + step, half) + side

    def origin(step):
        return lax.rem(group + half - step, half)

    def l_copy(i):
        c, b = i // NB, lax.rem(i, NB)
        return pltpu.make_async_copy(
            chol.at[pl.ds(pl.multiple_of(b * RB, RB), RB), pl.ds(pl.multiple_of(c * VC, VC), VC)],
            lbuf.at[lax.rem(i, RING)],
            l_sems.at[lax.rem(i, RING)],
        )

    def a_copy(b):
        return pltpu.make_async_copy(
            amplitudes.at[pl.ds(pl.multiple_of(b * RB, RB), RB), :], abuf.at[b], a_sems.at[b]
        )

    total = NC * NB
    shares = NT * (groups - 1)
    jobs = H * (shares + NT)

    def job_row(q):
        final = q >= H * shares
        k = lax.rem(q, shares)
        t = jnp.where(final, lax.rem(q - H * shares, NT), k // (groups - 1))
        d = jnp.where(final, 0, lax.rem(k, groups - 1) + 1)
        return lax.rem(vec + d, groups) * rows_out + t * TR

    def t_copy(q):
        slot = lax.rem(q, TILE_RING)
        return pltpu.make_async_copy(
            chol.at[pl.ds(pl.multiple_of(job_row(q), TR), TR), :], tiles.at[slot], t_sems.at[slot]
        )

    barrier = pltpu.get_barrier_semaphore()
    pl.semaphore_signal(barrier, inc=1, device_id={"ov": twin}, device_id_type=MESH)

    @pl.loop(1, half)
    def _(step):
        pl.semaphore_signal(barrier, inc=1, device_id={"ov": mate(step)}, device_id_type=MESH)

    @pl.loop(1, groups)
    def _(d):
        pl.semaphore_signal(
            barrier, inc=1, device_id={"vec": lax.rem(vec + d, groups)}, device_id_type=MESH
        )

    for b in range(NB):
        a_copy(b).start()
        if b < min(RING, total):
            l_copy(jnp.int32(b)).start()
    for i in range(NB, min(RING, total)):
        l_copy(jnp.int32(i)).start()

    def compute(c, first, last):
        @pl.loop(first, last)
        def _(b):
            i = c * NB + b
            if c == 0:
                a_copy(b).wait()
                at[b] = abuf[b].T
            l_copy(i).wait()
            acc[...] += jnp.dot(at[b], lbuf[lax.rem(i, RING)], preferred_element_type=jnp.float32)

            @pl.when(i + RING < total)
            def _():
                l_copy(i + RING).start()

    def store_part(c):
        for h in range(H):
            for vt in range(VT):
                block = acc[h * JW : (h + 1) * JW, vt * PV : (vt + 1) * PV]
                part[h, c, vt * JT : (vt + 1) * JT] = block.reshape(JT, JT_ROWS, PV)

    def to_ov(src, dst, send_sem, recv_sem, device):
        return pltpu.make_async_remote_copy(
            src_ref=src, dst_ref=dst, send_sem=send_sem, recv_sem=recv_sem,
            device_id={"ov": device}, device_id_type=MESH,
        )

    def swap(h, c):
        there = part.at[h, c, pl.ds((1 - side) * half, half)]
        return to_ov(there, paired.at[h, c], swap_s, swap_r.at[h, c], twin)

    def scatter(h, c, step):
        piece = halves.at[h, c, lax.rem(group + step, half)]
        return to_ov(piece, arrived.at[h, c, step - 1], scat_s, scat_r.at[h, c], mate(step))

    def gather(h, c, step):
        piece = coup.at[h, c, side * half + group]
        return to_ov(piece, piece, gath_s, gath_r.at[h, c], mate(step))

    def onward(h, c, hand):
        pieces = coup.at[h, c, pl.ds(hand * half, half)]
        return to_ov(pieces, pieces, on_s, on_r.at[h, c], twin)

    def all_scattered(h, c):
        return to_ov(arrived.at[h, c], arrived.at[h, c], scat_s, scat_r.at[h, c], twin)

    def all_gathered(h, c):
        pieces = coup.at[h, c, pl.ds(side * half, half - 1)]
        return to_ov(pieces, pieces, gath_s, gath_r.at[h, c], twin)

    def step1(h, c):
        swap(h, c).start()

    def step2(h, c):
        swap(h, c).wait_recv()

        @pl.loop(1, half)
        def _(step):
            piece = lax.rem(group + step, half)
            halves[h, c, piece] = (part[h, c, side * half + piece] + paired[h, c, piece]).astype(halves.dtype)
            scatter(h, c, step).start()

        own[h, c] = part[h, c, side * half + group] + paired[h, c, group]

    def step3(h, c):
        all_scattered(h, c).wait_recv()
        total = own[h, c]
        for step in range(1, half):
            total += arrived[h, c, step - 1].astype(jnp.float32)
        coup[h, c, side * half + group] = total.astype(coup.dtype)

        @pl.loop(1, half)
        def _(step):
            gather(h, c, step).start()

    def step4(h, c):
        all_gathered(h, c).wait_recv()
        onward(h, c, side).start()

    def step5(h, c):
        onward(h, c, 1 - side).wait_recv()
        for vt in range(VT):
            block = coup[h, c, vt * JT : (vt + 1) * JT].reshape(JW, PV)
            weights[h, c * VC + vt * PV : c * VC + (vt + 1) * PV, :] = block.T

    early, late = NB // 2, (3 * NB) // 4
    for c in range(NC):
        acc[...] = jnp.zeros_like(acc)
        compute(c, 0, early)
        if c >= 1:
            step2(0, c - 1)
        compute(c, early, late)
        if c >= 2:
            step3(0, c - 2)
        compute(c, late, NB)
        if c >= 3:
            step4(0, c - 3)
        store_part(c)
        if c == 0:
            pl.semaphore_wait(barrier, half + groups - 1)
        step1(0, c)

    for q in range(min(TILE_RING, jobs)):
        t_copy(jnp.int32(q)).start()
    p_copy = pltpu.make_async_copy(prior, pbuf, p_sem)
    p_copy.start()

    step2(0, NC - 1)
    if NC >= 2:
        step3(0, NC - 2)
    if NC >= 3:
        step4(0, NC - 3)
    for c in range(NC - 2):
        step5(0, c)
    step3(0, NC - 1)
    if NC >= 2:
        step4(0, NC - 2)
        step5(0, NC - 2)
    step4(0, NC - 1)
    step5(0, NC - 1)

    def x_copy(h, d, t, target):
        return pltpu.make_async_remote_copy(
            src_ref=sbuf.at[h, d - 1, t],
            dst_ref=rbuf.at[h, d - 1, t],
            send_sem=x_s,
            recv_sem=x_r.at[h, d - 1, t],
            device_id={"vec": target},
            device_id_type=MESH,
        )

    def tile_product(h, q):
        t_copy(q).wait()
        product = jnp.dot(
            tiles[lax.rem(q, TILE_RING)], weights[h], preferred_element_type=jnp.float32
        )
        return product

    def refill(q):
        @pl.when(q + TILE_RING < jobs)
        def _():
            t_copy(q + TILE_RING).start()

    def share_tiles(h, first, last):
        @pl.loop(first, last)
        def _(t):
            for d in range(1, groups):
                q = h * shares + t * (groups - 1) + d - 1
                sbuf[h, d - 1, t] = tile_product(h, q).astype(sbuf.dtype)
                x_copy(h, d, t, lax.rem(vec + d, groups)).start()
                refill(q)

    def final_tiles(h):
        @pl.loop(0, NT)
        def _(t):
            q = H * shares + h * NT + t
            total_tile = tile_product(h, q)
            refill(q)
            rows = pl.ds(pl.multiple_of(t * TR, TR), TR)
            columns = slice(h * JW, (h + 1) * JW)
            for d in range(1, groups):
                x_copy(h, d, t, lax.rem(vec + d, groups)).wait_recv()
                total_tile += rbuf[h, d - 1, t].astype(jnp.float32)
            out[rows, columns] = (pbuf[rows, columns].astype(jnp.float32) + total_tile).astype(out.dtype)

    for h in range(H):
        if h + 1 < H:
            for c in range(NC):
                step1(h + 1, c)
            edges = [0, NT // 8, NT // 2, (3 * NT) // 4, NT]
            for k, run in enumerate((step2, step3, step4, step5)):
                share_tiles(h, edges[k], edges[k + 1])
                for c in range(NC):
                    run(h + 1, c)
        else:
            share_tiles(h, 0, NT)
    p_copy.wait()
    for h in range(H):
        final_tiles(h)

    to_ov(paired, paired, swap_s, swap_r.at[0, 0], twin).wait_send()
    to_ov(arrived, arrived, scat_s, scat_r.at[0, 0], twin).wait_send()
    to_ov(arrived, arrived, gath_s, gath_r.at[0, 0], twin).wait_send()
    to_ov(halves, halves, on_s, on_r.at[0, 0], twin).wait_send()
    to_ov(sbuf, sbuf, x_s, x_r.at[0, 0, 0], twin).wait_send()


def body(n, groups, chol, amplitudes, prior):
    rows, vectors = chol.shape
    columns = amplitudes.shape[1]
    half = n // 2
    VC = divisor(vectors, (CHUNK, 256, 128))
    H = 2 if VC * (columns // 2) // JT_ROWS // n >= 128 else 1
    NC = vectors // VC
    RB = halved(rows, 4096)
    NB = rows // RB
    JW = columns // H
    PV = VC * (JW // JT_ROWS) // n
    TR = divisor(prior.shape[0], (256, 128, 64, 32, 16))
    NT = prior.shape[0] // TR
    plan = (n, groups, H, NC, NB, RB, VC, PV, JW, TR, NT)
    bf16, f32 = jnp.bfloat16, jnp.float32
    dma = pltpu.SemaphoreType.DMA
    return pl.pallas_call(
        functools.partial(kernel, plan),
        out_shape=pltpu.VMEM(prior.shape, prior.dtype),
        in_specs=[pl.BlockSpec(memory_space=pl.ANY)] * 3,
        out_specs=pl.BlockSpec(memory_space=pltpu.VMEM),
        scratch_shapes=[
            pltpu.VMEM((NB, RB, columns), bf16),
            pltpu.VMEM((NB, columns, RB), bf16),
            pltpu.VMEM((RING, RB, VC), bf16),
            pltpu.VMEM((columns, VC), f32),
            pltpu.VMEM((H, NC, n, JT_ROWS, PV), f32),
            pltpu.VMEM((H, NC, half, JT_ROWS, PV), f32),
            pltpu.VMEM((H, NC, half, JT_ROWS, PV), bf16),
            pltpu.VMEM((H, NC, half - 1, JT_ROWS, PV), bf16),
            pltpu.VMEM((H, NC, JT_ROWS, PV), f32),
            pltpu.VMEM((H, NC, n, JT_ROWS, PV), bf16),
            pltpu.VMEM((H, vectors, JW), bf16),
            pltpu.VMEM((TILE_RING, TR, vectors), bf16),
            pltpu.VMEM((H, groups - 1, NT, TR, JW), bf16),
            pltpu.VMEM((H, groups - 1, NT, TR, JW), bf16),
            pltpu.VMEM(prior.shape, bf16),
            dma((NB,)),
            dma((RING,)),
            dma((TILE_RING,)),
            dma(()),
            dma(()),
            dma((H, NC)),
            dma(()),
            dma((H, NC)),
            dma(()),
            dma((H, NC)),
            dma(()),
            dma((H, NC)),
            dma(()),
            dma((H, groups - 1, NT)),
        ],
        compiler_params=pltpu.CompilerParams(
            collective_id=0, has_side_effects=True, vmem_limit_bytes=54 * 2**20
        ),
    )(chol, amplitudes, prior)


def solution(mesh):
    return jax.shard_map(
        functools.partial(body, mesh.shape["ov"], mesh.shape["vec"]),
        mesh=mesh,
        in_specs=(P("ov", "vec"), P("ov", None), P(("ov", "vec"), None)),
        out_specs=P(("ov", "vec"), None),
        check_vma=False,
    )
```

```python
import functools

import jax
import jax.numpy as jnp
from jax import lax
from jax.experimental import pallas as pl
from jax.experimental.pallas import tpu as pltpu
from jax.sharding import PartitionSpec as P

MESH = pl.DeviceIdType.MESH
JT_ROWS = 16
CHUNK = 512
RING = 3
TILE_RING = 6


def halved(size, most):
    while size > most and size % 2 == 0:
        size //= 2
    return size


def divisor(size, choices):
    for choice in choices:
        if size % choice == 0:
            return choice
    return size


def kernel(
    plan, chol, amplitudes, prior, out,
    abuf, at, lbuf, acc, part, paired, halves, arrived, own, coup, weights, tiles, sbuf, rbuf, pbuf, raw, coup2, weights2,
    a_sems, l_sems, t_sems, p_sem, swap_s, swap_r, scat_s, scat_r, gath_s, gath_r, on_s, on_r, x_s, x_r,
    raw_s, raw_r, cross_s, cross_r, gath2_s, gath2_r, on2_s, on2_r,
):
    n, groups, H, NC, NB, RB, VC, PV, JW, TR, NT, NS = plan
    half = n // 2
    me = lax.axis_index("ov")
    vec = lax.axis_index("vec")
    side = lax.rem(me, 2)
    group = me // 2
    twin = me + 1 - 2 * side
    rows_out = TR * NT
    JT = JW // JT_ROWS
    VT = n // JT

    def mate(step):
        return 2 * lax.rem(group + step, half) + side

    def origin(step):
        return lax.rem(group + half - step, half)

    def l_copy(i):
        c, b = i // NB, lax.rem(i, NB)
        return pltpu.make_async_copy(
            chol.at[pl.ds(pl.multiple_of(b * RB, RB), RB), pl.ds(pl.multiple_of(c * VC, VC), VC)],
            lbuf.at[lax.rem(i, RING)],
            l_sems.at[lax.rem(i, RING)],
        )

    def a_copy(b):
        return pltpu.make_async_copy(
            amplitudes.at[pl.ds(pl.multiple_of(b * RB, RB), RB), :], abuf.at[b], a_sems.at[b]
        )

    total = NC * NB
    shares = NS * (groups - 1)
    jobs = H * (shares + NT)
    early_rows = NS < NT

    def final_tile_of(h, i):
        return jnp.where(h > 0, lax.rem(i + NS, NT), i)

    def job_row(q):
        final = q >= H * shares
        k = lax.rem(q, shares)
        i = q - H * shares
        t = jnp.where(final, final_tile_of(i // NT, lax.rem(i, NT)), k // (groups - 1))
        d = jnp.where(final, 0, lax.rem(k, groups - 1) + 1)
        return lax.rem(vec + d, groups) * rows_out + t * TR

    def t_copy(q):
        slot = lax.rem(q, TILE_RING)
        return pltpu.make_async_copy(
            chol.at[pl.ds(pl.multiple_of(job_row(q), TR), TR), :], tiles.at[slot], t_sems.at[slot]
        )

    barrier = pltpu.get_barrier_semaphore()
    pl.semaphore_signal(barrier, inc=1, device_id={"ov": twin}, device_id_type=MESH)

    @pl.loop(1, half)
    def _(step):
        pl.semaphore_signal(barrier, inc=1, device_id={"ov": mate(step)}, device_id_type=MESH)

    @pl.loop(1, groups)
    def _(d):
        pl.semaphore_signal(
            barrier, inc=1, device_id={"vec": lax.rem(vec + d, groups)}, device_id_type=MESH
        )

    for b in range(NB):
        a_copy(b).start()
        if b < min(RING, total):
            l_copy(jnp.int32(b)).start()
    for i in range(NB, min(RING, total)):
        l_copy(jnp.int32(i)).start()

    def compute(c, first, last):
        @pl.loop(first, last)
        def _(b):
            i = c * NB + b
            if c == 0:
                a_copy(b).wait()
                at[b] = abuf[b].T
            l_copy(i).wait()
            acc[...] += jnp.dot(at[b], lbuf[lax.rem(i, RING)], preferred_element_type=jnp.float32)

            @pl.when(i + RING < total)
            def _():
                l_copy(i + RING).start()

    def store_part(c):
        for h in range(H):
            for vt in range(VT):
                block = acc[h * JW : (h + 1) * JW, vt * PV : (vt + 1) * PV]
                part[h, c, vt * JT : (vt + 1) * JT] = block.reshape(JT, JT_ROWS, PV)

    def to_ov(src, dst, send_sem, recv_sem, device):
        return pltpu.make_async_remote_copy(
            src_ref=src, dst_ref=dst, send_sem=send_sem, recv_sem=recv_sem,
            device_id={"ov": device}, device_id_type=MESH,
        )

    def swap(h, c):
        there = part.at[h, c, pl.ds((1 - side) * half, half)]
        return to_ov(there, paired.at[h, c], swap_s, swap_r.at[h, c], twin)

    def scatter(h, c, step):
        piece = halves.at[h, c, lax.rem(group + step, half)]
        return to_ov(piece, arrived.at[h, c, step - 1], scat_s, scat_r.at[h, c], mate(step))

    def gather(h, c, step):
        piece = coup.at[h, c, side * half + group]
        return to_ov(piece, piece, gath_s, gath_r.at[h, c], mate(step))

    def onward(h, c, hand):
        pieces = coup.at[h, c, pl.ds(hand * half, half)]
        return to_ov(pieces, pieces, on_s, on_r.at[h, c], twin)

    def all_scattered(h, c):
        return to_ov(arrived.at[h, c], arrived.at[h, c], scat_s, scat_r.at[h, c], twin)

    def all_gathered(h, c):
        pieces = coup.at[h, c, pl.ds(side * half, half - 1)]
        return to_ov(pieces, pieces, gath_s, gath_r.at[h, c], twin)

    def step1(h, c):
        swap(h, c).start()

    def step2(h, c):
        swap(h, c).wait_recv()

        @pl.loop(1, half)
        def _(step):
            piece = lax.rem(group + step, half)
            halves[h, c, piece] = (part[h, c, side * half + piece] + paired[h, c, piece]).astype(halves.dtype)
            scatter(h, c, step).start()

        own[h, c] = part[h, c, side * half + group] + paired[h, c, group]

    def step3(h, c):
        all_scattered(h, c).wait_recv()
        total = own[h, c]
        for step in range(1, half):
            total += arrived[h, c, step - 1].astype(jnp.float32)
        coup[h, c, side * half + group] = total.astype(coup.dtype)
        if early_rows:
            cross(h, c).start()

        @pl.loop(1, half)
        def _(step):
            gather(h, c, step).start()

    def step4(h, c):
        all_gathered(h, c).wait_recv()
        onward(h, c, side).start()

    def step5(h, c):
        onward(h, c, 1 - side).wait_recv()
        for vt in range(VT):
            block = coup[h, c, vt * JT : (vt + 1) * JT].reshape(JW, PV)
            weights[h, c * VC + vt * PV : c * VC + (vt + 1) * PV, :] = block.T

    other = lax.rem(vec + 1, groups)
    def raw_copy():
        return pltpu.make_async_remote_copy(
            src_ref=chol.at[pl.ds(pl.multiple_of(other * rows_out + (NT - 1) * TR, TR), TR), :],
            dst_ref=raw,
            send_sem=raw_s,
            recv_sem=raw_r,
            device_id={"vec": other},
            device_id_type=MESH,
        )

    def cross(h, c):
        return pltpu.make_async_remote_copy(
            src_ref=coup.at[h, c, side * half + group],
            dst_ref=coup2.at[h, c, side * half + group],
            send_sem=cross_s.at[h, c],
            recv_sem=cross_r.at[h, c],
            device_id={"vec": other},
            device_id_type=MESH,
        )

    def step6(h, c):
        cross(h, c).wait_recv()

        @pl.loop(1, half)
        def _(step):
            piece = coup2.at[h, c, side * half + group]
            to_ov(piece, piece, gath2_s, gath2_r.at[h, c], mate(step)).start()

    def onward2(h, c, hand):
        pieces = coup2.at[h, c, pl.ds(hand * half, half)]
        return to_ov(pieces, pieces, on2_s, on2_r.at[h, c], twin)

    def step7(h, c):
        pieces = coup2.at[h, c, pl.ds(side * half, half - 1)]
        to_ov(pieces, pieces, gath2_s, gath2_r.at[h, c], twin).wait_recv()
        onward2(h, c, side).start()

    def step8(h, c):
        onward2(h, c, 1 - side).wait_recv()
        for vt in range(VT):
            block = coup2[h, c, vt * JT : (vt + 1) * JT].reshape(JW, PV)
            weights2[h, c * VC + vt * PV : c * VC + (vt + 1) * PV, :] = block.T

    early, late = NB // 2, (3 * NB) // 4
    for c in range(NC):
        acc[...] = jnp.zeros_like(acc)
        compute(c, 0, early)
        if c >= 1:
            step2(0, c - 1)
        compute(c, early, late)
        if c >= 2:
            step3(0, c - 2)
        compute(c, late, NB)
        if c >= 3:
            step4(0, c - 3)
        store_part(c)
        if c == 0:
            pl.semaphore_wait(barrier, half + groups - 1)
            if early_rows:
                raw_copy().start()
        step1(0, c)

    for q in range(min(TILE_RING, jobs)):
        t_copy(jnp.int32(q)).start()
    p_copy = pltpu.make_async_copy(prior, pbuf, p_sem)
    p_copy.start()

    step2(0, NC - 1)
    if NC >= 2:
        step3(0, NC - 2)
    if NC >= 3:
        step4(0, NC - 3)
    for c in range(NC - 2):
        step5(0, c)
    step3(0, NC - 1)
    if NC >= 2:
        step4(0, NC - 2)
        step5(0, NC - 2)
    step4(0, NC - 1)
    step5(0, NC - 1)

    def x_copy(h, d, t, target):
        return pltpu.make_async_remote_copy(
            src_ref=sbuf.at[h, d - 1, t],
            dst_ref=rbuf.at[h, d - 1, t],
            send_sem=x_s,
            recv_sem=x_r.at[h, d - 1, t],
            device_id={"vec": target},
            device_id_type=MESH,
        )

    def tile_product(h, q):
        t_copy(q).wait()
        product = jnp.dot(
            tiles[lax.rem(q, TILE_RING)], weights[h], preferred_element_type=jnp.float32
        )
        return product

    def refill(q):
        @pl.when(q + TILE_RING < jobs)
        def _():
            t_copy(q + TILE_RING).start()

    def share_tiles(h, first, last):
        @pl.loop(first, last)
        def _(t):
            for d in range(1, groups):
                q = h * shares + t * (groups - 1) + d - 1
                sbuf[h, d - 1, t] = tile_product(h, q).astype(sbuf.dtype)
                x_copy(h, d, t, lax.rem(vec + d, groups)).start()
                refill(q)

    def final_tile(h, i, with_raw):
        q = H * shares + h * NT + i
        t = final_tile_of(h, i)
        total_tile = tile_product(h, q)
        refill(q)
        rows = pl.ds(pl.multiple_of(t * TR, TR), TR)
        columns = slice(h * JW, (h + 1) * JW)
        if with_raw:
            total_tile += jnp.dot(raw[...], weights2[h], preferred_element_type=jnp.float32)
        else:
            for d in range(1, groups):
                x_copy(h, d, t, lax.rem(vec + d, groups)).wait_recv()
                total_tile += rbuf[h, d - 1, t].astype(jnp.float32)
        out[rows, columns] = (pbuf[rows, columns].astype(jnp.float32) + total_tile).astype(out.dtype)

    def final_tiles(h, first, last):
        @pl.loop(first, last)
        def _(i):
            final_tile(h, i, False)

    for h in range(H):
        if h + 1 < H:
            for c in range(NC):
                step1(h + 1, c)
            edges = [0, NS // 8, NS // 2, (3 * NS) // 4, NS]
            for k, run in enumerate((step2, step3, step4, step5)):
                share_tiles(h, edges[k], edges[k + 1])
                for c in range(NC):
                    run(h + 1, c)
        else:
            share_tiles(h, 0, NS)
    p_copy.wait()
    every = [(h, c) for h in range(H) for c in range(NC)]
    if early_rows:
        for h, c in every:
            step6(h, c)
        final_tiles(0, 0, NT // 2)
        for h, c in every:
            step7(h, c)
        final_tiles(0, NT // 2, NS)
        for h, c in every:
            step8(h, c)
        raw_copy().wait_recv()
        final_tile(0, jnp.int32(NS), True)
        for h in range(1, H):
            final_tile(h, jnp.int32(0), True)
            final_tiles(h, 1, NT)
    else:
        for h in range(H):
            final_tiles(h, 0, NT)

    to_ov(paired, paired, swap_s, swap_r.at[0, 0], twin).wait_send()
    to_ov(arrived, arrived, scat_s, scat_r.at[0, 0], twin).wait_send()
    to_ov(arrived, arrived, gath_s, gath_r.at[0, 0], twin).wait_send()
    to_ov(halves, halves, on_s, on_r.at[0, 0], twin).wait_send()
    to_ov(sbuf, sbuf, x_s, x_r.at[0, 0, 0], twin).wait_send()
    if early_rows:
        raw_copy().wait_send()
        for h, c in every:
            cross(h, c).wait_send()
        to_ov(arrived, arrived, gath2_s, gath2_r.at[0, 0], twin).wait_send()
        to_ov(halves, halves, on2_s, on2_r.at[0, 0], twin).wait_send()


def body(n, groups, chol, amplitudes, prior):
    rows, vectors = chol.shape
    columns = amplitudes.shape[1]
    half = n // 2
    VC = divisor(vectors, (CHUNK, 256, 128))
    H = 2 if VC * (columns // 2) // JT_ROWS // n >= 128 else 1
    NC = vectors // VC
    RB = halved(rows, 4096)
    NB = rows // RB
    JW = columns // H
    PV = VC * (JW // JT_ROWS) // n
    TR = divisor(prior.shape[0], (256, 128, 64, 32, 16))
    NT = prior.shape[0] // TR
    NS = NT - 1 if groups == 2 and NT > 2 else NT
    plan = (n, groups, H, NC, NB, RB, VC, PV, JW, TR, NT, NS)
    bf16, f32 = jnp.bfloat16, jnp.float32
    dma = pltpu.SemaphoreType.DMA
    return pl.pallas_call(
        functools.partial(kernel, plan),
        out_shape=pltpu.VMEM(prior.shape, prior.dtype),
        in_specs=[pl.BlockSpec(memory_space=pl.ANY)] * 3,
        out_specs=pl.BlockSpec(memory_space=pltpu.VMEM),
        scratch_shapes=[
            pltpu.VMEM((NB, RB, columns), bf16),
            pltpu.VMEM((NB, columns, RB), bf16),
            pltpu.VMEM((RING, RB, VC), bf16),
            pltpu.VMEM((columns, VC), f32),
            pltpu.VMEM((H, NC, n, JT_ROWS, PV), f32),
            pltpu.VMEM((H, NC, half, JT_ROWS, PV), f32),
            pltpu.VMEM((H, NC, half, JT_ROWS, PV), bf16),
            pltpu.VMEM((H, NC, half - 1, JT_ROWS, PV), bf16),
            pltpu.VMEM((H, NC, JT_ROWS, PV), f32),
            pltpu.VMEM((H, NC, n, JT_ROWS, PV), bf16),
            pltpu.VMEM((H, vectors, JW), bf16),
            pltpu.VMEM((TILE_RING, TR, vectors), bf16),
            pltpu.VMEM((H, groups - 1, NS, TR, JW), bf16),
            pltpu.VMEM((H, groups - 1, NS, TR, JW), bf16),
            pltpu.VMEM(prior.shape, bf16),
            pltpu.VMEM((TR, vectors), bf16),
            pltpu.VMEM((H, NC, n, JT_ROWS, PV), bf16),
            pltpu.VMEM((H, vectors, JW), bf16),
            dma((NB,)),
            dma((RING,)),
            dma((TILE_RING,)),
            dma(()),
            dma(()),
            dma((H, NC)),
            dma(()),
            dma((H, NC)),
            dma(()),
            dma((H, NC)),
            dma(()),
            dma((H, NC)),
            dma(()),
            dma((H, groups - 1, NS)),
            dma(()),
            dma(()),
            dma((H, NC)),
            dma((H, NC)),
            dma(()),
            dma((H, NC)),
            dma(()),
            dma((H, NC)),
        ],
        compiler_params=pltpu.CompilerParams(
            collective_id=0, has_side_effects=True, vmem_limit_bytes=54 * 2**20
        ),
    )(chol, amplitudes, prior)


def solution(mesh):
    return jax.shard_map(
        functools.partial(body, mesh.shape["ov"], mesh.shape["vec"]),
        mesh=mesh,
        in_specs=(P("ov", "vec"), P("ov", None), P(("ov", "vec"), None)),
        out_specs=P(("ov", "vec"), None),
        check_vma=False,
    )
```

```python
import functools

import jax
import jax.numpy as jnp
from jax import lax
from jax.experimental import pallas as pl
from jax.experimental.pallas import tpu as pltpu
from jax.sharding import PartitionSpec as P

MESH = pl.DeviceIdType.MESH
JT_ROWS = 16
CHUNK = 512
RING = 3
TILE_RING = 6


def halved(size, most):
    while size > most and size % 2 == 0:
        size //= 2
    return size


def divisor(size, choices):
    for choice in choices:
        if size % choice == 0:
            return choice
    return size


def kernel(
    plan, chol, amplitudes, prior, out,
    abuf, at, lbuf, acc, part, paired, halves, arrived, own, coup, weights, tiles, sbuf, rbuf, pbuf, raw, coup2, weights2,
    a_sems, l_sems, t_sems, p_sem, swap_s, swap_r, scat_s, scat_r, gath_s, gath_r, on_s, on_r, x_s, x_r,
    raw_s, raw_r, cross_s, cross_r, gath2_s, gath2_r, on2_s, on2_r,
):
    n, groups, H, NC, NB, RB, VC, PV, JW, TR, NT, NS = plan
    half = n // 2
    me = lax.axis_index("ov")
    vec = lax.axis_index("vec")
    side = lax.rem(me, 2)
    group = me // 2
    twin = me + 1 - 2 * side
    rows_out = TR * NT
    JT = JW // JT_ROWS
    VT = n // JT

    def mate(step):
        return 2 * lax.rem(group + step, half) + side

    def origin(step):
        return lax.rem(group + half - step, half)

    def l_copy(i):
        c, b = i // NB, lax.rem(i, NB)
        return pltpu.make_async_copy(
            chol.at[pl.ds(pl.multiple_of(b * RB, RB), RB), pl.ds(pl.multiple_of(c * VC, VC), VC)],
            lbuf.at[lax.rem(i, RING)],
            l_sems.at[lax.rem(i, RING)],
        )

    def a_copy(b):
        return pltpu.make_async_copy(
            amplitudes.at[pl.ds(pl.multiple_of(b * RB, RB), RB), :], abuf.at[b], a_sems.at[b]
        )

    total = NC * NB
    shares = NS * (groups - 1)
    jobs = H * (shares + NT)
    early_rows = NS < NT

    def final_tile_of(h, i):
        return jnp.where(h > 0, lax.rem(i + NS, NT), i)

    def job_row(q):
        final = q >= H * shares
        k = lax.rem(q, shares)
        i = q - H * shares
        t = jnp.where(final, final_tile_of(i // NT, lax.rem(i, NT)), k // (groups - 1))
        d = jnp.where(final, 0, lax.rem(k, groups - 1) + 1)
        return lax.rem(vec + d, groups) * rows_out + t * TR

    def t_copy(q):
        slot = lax.rem(q, TILE_RING)
        return pltpu.make_async_copy(
            chol.at[pl.ds(pl.multiple_of(job_row(q), TR), TR), :], tiles.at[slot], t_sems.at[slot]
        )

    barrier = pltpu.get_barrier_semaphore()
    pl.semaphore_signal(barrier, inc=1, device_id={"ov": twin}, device_id_type=MESH)

    @pl.loop(1, half)
    def _(step):
        pl.semaphore_signal(barrier, inc=1, device_id={"ov": mate(step)}, device_id_type=MESH)

    @pl.loop(1, groups)
    def _(d):
        pl.semaphore_signal(
            barrier, inc=1, device_id={"vec": lax.rem(vec + d, groups)}, device_id_type=MESH
        )

    for b in range(NB):
        a_copy(b).start()
        if b < min(RING, total):
            l_copy(jnp.int32(b)).start()
    for i in range(NB, min(RING, total)):
        l_copy(jnp.int32(i)).start()

    def compute(c, first, last):
        @pl.loop(first, last)
        def _(b):
            i = c * NB + b
            if c == 0:
                a_copy(b).wait()
                at[b] = abuf[b].T
            l_copy(i).wait()
            acc[...] += jnp.dot(at[b], lbuf[lax.rem(i, RING)], preferred_element_type=jnp.float32)

            @pl.when(i + RING < total)
            def _():
                l_copy(i + RING).start()

    def store_part(c):
        for h in range(H):
            for vt in range(VT):
                block = acc[h * JW : (h + 1) * JW, vt * PV : (vt + 1) * PV]
                part[h, c, vt * JT : (vt + 1) * JT] = block.reshape(JT, JT_ROWS, PV)

    def to_ov(src, dst, send_sem, recv_sem, device):
        return pltpu.make_async_remote_copy(
            src_ref=src, dst_ref=dst, send_sem=send_sem, recv_sem=recv_sem,
            device_id={"ov": device}, device_id_type=MESH,
        )

    def swap(h, c):
        there = part.at[h, c, pl.ds((1 - side) * half, half)]
        return to_ov(there, paired.at[h, c], swap_s, swap_r.at[h, c], twin)

    def scatter(h, c, step):
        piece = halves.at[h, c, lax.rem(group + step, half)]
        return to_ov(piece, arrived.at[h, c, step - 1], scat_s, scat_r.at[h, c], mate(step))

    def gather(h, c, step):
        piece = coup.at[h, c, side * half + group]
        return to_ov(piece, piece, gath_s, gath_r.at[h, c], mate(step))

    def onward(h, c, hand):
        pieces = coup.at[h, c, pl.ds(hand * half, half)]
        return to_ov(pieces, pieces, on_s, on_r.at[h, c], twin)

    def all_scattered(h, c):
        return to_ov(arrived.at[h, c], arrived.at[h, c], scat_s, scat_r.at[h, c], twin)

    def all_gathered(h, c):
        pieces = coup.at[h, c, pl.ds(side * half, half - 1)]
        return to_ov(pieces, pieces, gath_s, gath_r.at[h, c], twin)

    def step1(h, c):
        swap(h, c).start()

    def step2(h, c):
        swap(h, c).wait_recv()

        @pl.loop(1, half)
        def _(step):
            piece = lax.rem(group + step, half)
            halves[h, c, piece] = (part[h, c, side * half + piece] + paired[h, c, piece]).astype(halves.dtype)
            scatter(h, c, step).start()

        own[h, c] = part[h, c, side * half + group] + paired[h, c, group]

    def step3(h, c):
        all_scattered(h, c).wait_recv()
        total = own[h, c]
        for step in range(1, half):
            total += arrived[h, c, step - 1].astype(jnp.float32)
        coup[h, c, side * half + group] = total.astype(coup.dtype)

        @pl.loop(1, half)
        def _(step):
            gather(h, c, step).start()

        if early_rows:
            cross(h, c).start()

    def step4(h, c):
        all_gathered(h, c).wait_recv()
        onward(h, c, side).start()

    def step5(h, c):
        onward(h, c, 1 - side).wait_recv()
        for vt in range(VT):
            block = coup[h, c, vt * JT : (vt + 1) * JT].reshape(JW, PV)
            weights[h, c * VC + vt * PV : c * VC + (vt + 1) * PV, :] = block.T

    other = lax.rem(vec + 1, groups)
    def raw_copy():
        return pltpu.make_async_remote_copy(
            src_ref=chol.at[pl.ds(pl.multiple_of(other * rows_out + (NT - 1) * TR, TR), TR), :],
            dst_ref=raw,
            send_sem=raw_s,
            recv_sem=raw_r,
            device_id={"vec": other},
            device_id_type=MESH,
        )

    def cross(h, c):
        return pltpu.make_async_remote_copy(
            src_ref=coup.at[h, c, side * half + group],
            dst_ref=coup2.at[h, c, side * half + group],
            send_sem=cross_s.at[h, c],
            recv_sem=cross_r.at[h, c],
            device_id={"vec": other},
            device_id_type=MESH,
        )

    def step6(h, c):
        cross(h, c).wait_recv()

        @pl.loop(1, half)
        def _(step):
            piece = coup2.at[h, c, side * half + group]
            to_ov(piece, piece, gath2_s, gath2_r.at[h, c], mate(step)).start()

    def onward2(h, c, hand):
        pieces = coup2.at[h, c, pl.ds(hand * half, half)]
        return to_ov(pieces, pieces, on2_s, on2_r.at[h, c], twin)

    def step7(h, c):
        pieces = coup2.at[h, c, pl.ds(side * half, half - 1)]
        to_ov(pieces, pieces, gath2_s, gath2_r.at[h, c], twin).wait_recv()
        onward2(h, c, side).start()

    def step8(h, c):
        onward2(h, c, 1 - side).wait_recv()
        for vt in range(VT):
            block = coup2[h, c, vt * JT : (vt + 1) * JT].reshape(JW, PV)
            weights2[h, c * VC + vt * PV : c * VC + (vt + 1) * PV, :] = block.T

    early, late = NB // 2, (3 * NB) // 4
    for c in range(NC):
        acc[...] = jnp.zeros_like(acc)
        compute(c, 0, early)
        if c >= 1:
            step2(0, c - 1)
        compute(c, early, late)
        if c >= 2:
            step3(0, c - 2)
        compute(c, late, NB)
        if c >= 3:
            step4(0, c - 3)
        store_part(c)
        if c == 0:
            pl.semaphore_wait(barrier, half + groups - 1)
            if early_rows:
                raw_copy().start()
        step1(0, c)

    for q in range(min(TILE_RING, jobs)):
        t_copy(jnp.int32(q)).start()
    p_copy = pltpu.make_async_copy(prior, pbuf, p_sem)
    p_copy.start()

    step2(0, NC - 1)
    if NC >= 2:
        step3(0, NC - 2)
    if NC >= 3:
        step4(0, NC - 3)
    for c in range(NC - 2):
        step5(0, c)
    step3(0, NC - 1)
    if NC >= 2:
        step4(0, NC - 2)
        step5(0, NC - 2)
    step4(0, NC - 1)
    known = (NC - 1) * VC
    ahead = NC > 1 and NS // 8 > 1 and H > 1 and groups == 2 and TR <= acc.shape[0]
    if ahead:
        t_copy(jnp.int32(0)).wait()
        acc[:TR, :JW] = jnp.dot(
            tiles[0, :, :known], weights[0, :known], preferred_element_type=jnp.float32
        )
    step5(0, NC - 1)

    def x_copy(h, d, t, target):
        return pltpu.make_async_remote_copy(
            src_ref=sbuf.at[h, d - 1, t],
            dst_ref=rbuf.at[h, d - 1, t],
            send_sem=x_s,
            recv_sem=x_r.at[h, d - 1, t],
            device_id={"vec": target},
            device_id_type=MESH,
        )

    def tile_product(h, q):
        t_copy(q).wait()
        product = jnp.dot(
            tiles[lax.rem(q, TILE_RING)], weights[h], preferred_element_type=jnp.float32
        )
        return product

    def refill(q):
        @pl.when(q + TILE_RING < jobs)
        def _():
            t_copy(q + TILE_RING).start()

    def first_share():
        rest = jnp.dot(tiles[0, :, known:], weights[0, known:], preferred_element_type=jnp.float32)
        sbuf[0, 0, 0] = (acc[:TR, :JW] + rest).astype(sbuf.dtype)
        x_copy(0, 1, 0, lax.rem(vec + 1, groups)).start()
        refill(jnp.int32(0))

    def share_tiles(h, first, last):
        @pl.loop(first, last)
        def _(t):
            for d in range(1, groups):
                q = h * shares + t * (groups - 1) + d - 1
                sbuf[h, d - 1, t] = tile_product(h, q).astype(sbuf.dtype)
                x_copy(h, d, t, lax.rem(vec + d, groups)).start()
                refill(q)

    def final_tile(h, i, with_raw):
        q = H * shares + h * NT + i
        t = final_tile_of(h, i)
        total_tile = tile_product(h, q)
        refill(q)
        rows = pl.ds(pl.multiple_of(t * TR, TR), TR)
        columns = slice(h * JW, (h + 1) * JW)
        if with_raw:
            total_tile += jnp.dot(raw[...], weights2[h], preferred_element_type=jnp.float32)
        else:
            for d in range(1, groups):
                x_copy(h, d, t, lax.rem(vec + d, groups)).wait_recv()
                total_tile += rbuf[h, d - 1, t].astype(jnp.float32)
        out[rows, columns] = (pbuf[rows, columns].astype(jnp.float32) + total_tile).astype(out.dtype)

    def final_tiles(h, first, last):
        @pl.loop(first, last)
        def _(i):
            final_tile(h, i, False)

    if ahead:
        first_share()
    for h in range(H):
        if h + 1 < H:
            for c in range(NC):
                step1(h + 1, c)
            edges = [1 if h == 0 and ahead else 0, NS // 8, NS // 2, (3 * NS) // 4, NS]
            for k, run in enumerate((step2, step3, step4, step5)):
                share_tiles(h, edges[k], edges[k + 1])
                for c in range(NC):
                    run(h + 1, c)
        else:
            share_tiles(h, 0, NS)
    p_copy.wait()
    every = [(h, c) for h in range(H) for c in range(NC)]
    if early_rows:
        for h, c in every:
            step6(h, c)
        final_tiles(0, 0, NT // 2)
        for h, c in every:
            step7(h, c)
        final_tiles(0, NT // 2, NS)
        for h, c in every:
            step8(h, c)
        raw_copy().wait_recv()
        final_tile(0, jnp.int32(NS), True)
        for h in range(1, H):
            final_tile(h, jnp.int32(0), True)
            final_tiles(h, 1, NT)
    else:
        for h in range(H):
            final_tiles(h, 0, NT)

    to_ov(paired, paired, swap_s, swap_r.at[0, 0], twin).wait_send()
    to_ov(arrived, arrived, scat_s, scat_r.at[0, 0], twin).wait_send()
    to_ov(arrived, arrived, gath_s, gath_r.at[0, 0], twin).wait_send()
    to_ov(halves, halves, on_s, on_r.at[0, 0], twin).wait_send()
    to_ov(sbuf, sbuf, x_s, x_r.at[0, 0, 0], twin).wait_send()
    if early_rows:
        raw_copy().wait_send()
        for h, c in every:
            cross(h, c).wait_send()
        to_ov(arrived, arrived, gath2_s, gath2_r.at[0, 0], twin).wait_send()
        to_ov(halves, halves, on2_s, on2_r.at[0, 0], twin).wait_send()


def body(n, groups, chol, amplitudes, prior):
    rows, vectors = chol.shape
    columns = amplitudes.shape[1]
    half = n // 2
    VC = divisor(vectors, (CHUNK, 256, 128))
    H = 2 if VC * (columns // 2) // JT_ROWS // n >= 128 else 1
    NC = vectors // VC
    RB = halved(rows, 4096)
    NB = rows // RB
    JW = columns // H
    PV = VC * (JW // JT_ROWS) // n
    TR = divisor(prior.shape[0], (256, 128, 64, 32, 16))
    NT = prior.shape[0] // TR
    NS = NT - 1 if groups == 2 and NT > 2 else NT
    plan = (n, groups, H, NC, NB, RB, VC, PV, JW, TR, NT, NS)
    bf16, f32 = jnp.bfloat16, jnp.float32
    dma = pltpu.SemaphoreType.DMA
    return pl.pallas_call(
        functools.partial(kernel, plan),
        out_shape=pltpu.VMEM(prior.shape, prior.dtype),
        in_specs=[pl.BlockSpec(memory_space=pl.ANY)] * 3,
        out_specs=pl.BlockSpec(memory_space=pltpu.VMEM),
        scratch_shapes=[
            pltpu.VMEM((NB, RB, columns), bf16),
            pltpu.VMEM((NB, columns, RB), bf16),
            pltpu.VMEM((RING, RB, VC), bf16),
            pltpu.VMEM((columns, VC), f32),
            pltpu.VMEM((H, NC, n, JT_ROWS, PV), f32),
            pltpu.VMEM((H, NC, half, JT_ROWS, PV), f32),
            pltpu.VMEM((H, NC, half, JT_ROWS, PV), bf16),
            pltpu.VMEM((H, NC, half - 1, JT_ROWS, PV), bf16),
            pltpu.VMEM((H, NC, JT_ROWS, PV), f32),
            pltpu.VMEM((H, NC, n, JT_ROWS, PV), bf16),
            pltpu.VMEM((H, vectors, JW), bf16),
            pltpu.VMEM((TILE_RING, TR, vectors), bf16),
            pltpu.VMEM((H, groups - 1, NS, TR, JW), bf16),
            pltpu.VMEM((H, groups - 1, NS, TR, JW), bf16),
            pltpu.VMEM(prior.shape, bf16),
            pltpu.VMEM((TR, vectors), bf16),
            pltpu.VMEM((H, NC, n, JT_ROWS, PV), bf16),
            pltpu.VMEM((H, vectors, JW), bf16),
            dma((NB,)),
            dma((RING,)),
            dma((TILE_RING,)),
            dma(()),
            dma(()),
            dma((H, NC)),
            dma(()),
            dma((H, NC)),
            dma(()),
            dma((H, NC)),
            dma(()),
            dma((H, NC)),
            dma(()),
            dma((H, groups - 1, NS)),
            dma(()),
            dma(()),
            dma((H, NC)),
            dma((H, NC)),
            dma(()),
            dma((H, NC)),
            dma(()),
            dma((H, NC)),
        ],
        compiler_params=pltpu.CompilerParams(
            collective_id=0, has_side_effects=True, vmem_limit_bytes=54 * 2**20
        ),
    )(chol, amplitudes, prior)


def solution(mesh):
    return jax.shard_map(
        functools.partial(body, mesh.shape["ov"], mesh.shape["vec"]),
        mesh=mesh,
        in_specs=(P("ov", "vec"), P("ov", None), P(("ov", "vec"), None)),
        out_specs=P(("ov", "vec"), None),
        check_vma=False,
    )
```
